32 devices in a mesh: seq: 8 (over z, x), ch: 4 (over y, core).
Axes of the slice: x: 2, y: 2, z: 4, core: 2. Of those that a mesh axis runs over, the one named last changes fastest.
Arguments:
- values: float32 [2048, 1024], P('seq', 'ch'), may hold values from -6 to 6
- gates: float32 [2048, 1024], P('seq', 'ch'), may hold values from -6 to 6
- filter_taps: float32 [4096, 1024], P('seq', 'ch'), may hold values from -0.09375 to 0.09375
- skip: float32 [1024], P('ch'), may hold values from 0.5 to 2
- out_weight: bfloat16 [1024, 2048], P(None, 'ch'), may hold values from -0.1875 to 0.1875
Outputs:
- mixed: float32 [2048, 2048], P('seq', 'ch')
The draws below stay inside these ranges and needn't reach their ends.
All inputs are finite; a program needn't handle non-finite values.
Results may differ from the reference program's by a relative error of at most 0.0058.
Values may be sent and summed in bfloat16 or wider, within the bound.
A program may use at most 64 MiB of HBM per device.

```python
import jax
import jax.numpy as jnp

D = 2048
CHANNELS = 1024
FILTER = 4096
TOKENS = 2048


def shard_levels(key, dims, shards, low, top_value):
    factor_of, own = 1.0, jax.random.fold_in(key, 6)
    for position, parts in shards:
        steps = jnp.exp(jax.random.uniform(jax.random.fold_in(own, position), (parts,), jnp.float32, low / len(shards), top_value / len(shards)))
        factor_of = factor_of * jnp.repeat(steps, dims[position] // parts).reshape([-1 if axis == position else 1 for axis in range(len(dims))])
    return factor_of


def gaussian(rng, shape, deviation, bound, split=(), kind=jnp.bfloat16):
    loudness = shard_levels(rng, shape, split, -0.22, 0.18) if split else 1.0
    result = jax.random.normal(rng, shape, jnp.float32) * deviation * loudness
    return jnp.minimum(jnp.maximum(result, -bound), bound).astype(kind)


def setup_inputs(seed: int = 0) -> dict:
    arg_keys = jax.random.split(jax.random.key(seed), 6)
    return {
        "values": gaussian(arg_keys[0], (TOKENS, CHANNELS), 1.0, 6.0, ((0, 8), (1, 4)), jnp.float32),
        "gates": gaussian(arg_keys[1], (TOKENS, CHANNELS), 1.0, 6.0, ((0, 8), (1, 4)), jnp.float32),
        "filter_taps": gaussian(arg_keys[2], (FILTER, CHANNELS), FILTER ** -0.5, 0.09375, ((0, 8), (1, 4)), jnp.float32),
        "skip": jnp.clip(0.5 + 1.5 * jax.random.uniform(arg_keys[3], (CHANNELS,), jnp.float32) ** shard_levels(arg_keys[3], (CHANNELS,), ((0, 4),), -0.2, 0.2), 0.5, 2.0),
        "out_weight": gaussian(arg_keys[4], (CHANNELS, D), CHANNELS ** -0.5, 0.1875, ((1, 4),)),
    }


def reference(values, gates, filter_taps, skip, out_weight):
    length = values.shape[0]
    padded = 1 << (length + FILTER - 1).bit_length()
    spectrum = jnp.fft.rfft(values, n=padded, axis=0) * jnp.fft.rfft(filter_taps, n=padded, axis=0)
    convolved = jnp.fft.irfft(spectrum, n=padded, axis=0)[:length]
    hidden = (gates * (convolved + skip[None, :] * values)).astype(jnp.bfloat16)
    return jnp.dot(hidden, out_weight, preferred_element_type=jnp.float32)
```

```python
import functools
import math

import jax
import jax.numpy as jnp
from jax import lax
from jax.experimental import pallas as pl
from jax.experimental.pallas import tpu as pltpu
from jax.sharding import PartitionSpec as P

HIGHEST = lax.Precision.HIGHEST
MESH = pl.DeviceIdType.MESH
LANES = 128
TILE = 16


def split_length(length):
    leading = 1
    for factor in range(1, math.isqrt(length) + 1):
        if length % factor == 0:
            leading = factor
    return (leading, length // leading)


def phase_table(count_rows, count_cols, modulus):
    row_ids = jnp.arange(count_rows, dtype=jnp.int32)
    col_ids = jnp.arange(count_cols, dtype=jnp.int32)
    wrapped = row_ids[:, None] * col_ids[None, :] % modulus
    phases = 2.0 * math.pi / modulus * wrapped.astype(jnp.float32)
    return (jnp.cos(phases), jnp.sin(phases))


def complex_form(cosine, sine):
    upper = jnp.stack([cosine, -sine], axis=1)
    lower = jnp.stack([sine, cosine], axis=1)
    return jnp.stack([upper, lower], axis=0)


def transform_tables(length):
    rows_lead, rows_tail = split_length(length)
    cos_lead, sin_lead = phase_table(rows_lead, rows_lead, rows_lead)
    cos_tail, sin_tail = phase_table(rows_tail, rows_tail, rows_tail)
    cos_twist, sin_twist = phase_table(rows_lead, rows_tail, length)
    lead_table = jnp.stack([cos_lead, -sin_lead])
    tail_forward = complex_form(cos_tail, -sin_tail)
    tail_inverse = complex_form(cos_tail, sin_tail)
    return (
        lead_table,
        tail_forward,
        tail_inverse,
        cos_twist,
        sin_twist,
        rows_lead,
        rows_tail,
        length,
    )


def twist_rows(section, cosine, sine):
    real_part = section[0] * cosine[None] - section[1] * sine[None]
    imag_part = section[0] * sine[None] + section[1] * cosine[None]
    return jnp.stack([real_part, imag_part])


def forward_rows(rows, tables):
    lead_table, tail_forward, tail_inverse, cos_twist, sin_twist, rows_lead, rows_tail, length = (
        tables
    )
    signal = jnp.concatenate([rows, jnp.zeros_like(rows)], axis=1).reshape(
        rows.shape[0], rows_lead, rows_tail
    )
    section = jnp.einsum("pft,cts->pcfs", lead_table, signal, precision=HIGHEST)
    twisted = twist_rows(section, cos_twist, -sin_twist)
    return jnp.einsum("pgrs,rcfs->pcfg", tail_forward, twisted, precision=HIGHEST)


def inverse_rows(spectrum, tables):
    lead_table, tail_forward, tail_inverse, cos_twist, sin_twist, rows_lead, rows_tail, length = (
        tables
    )
    section = jnp.einsum("pgrs,rcfs->pcfg", tail_inverse, spectrum, precision=HIGHEST)
    twisted = twist_rows(section, cos_twist, sin_twist)
    signal = jnp.einsum("rft,rcfs->cts", lead_table, twisted, precision=HIGHEST) / length
    return signal.reshape(signal.shape[0], length)


def product(left, right):
    real_part = left[0] * right[0] - left[1] * right[1]
    imag_part = left[0] * right[1] + left[1] * right[0]
    return jnp.stack([real_part, imag_part])


def body(values, gates, filter_taps, skip, out_weight):
    block_rows, width = values.shape
    whole_filter = lax.all_gather(filter_taps, "seq", axis=0, tiled=True)
    devices = lax.axis_size("seq")
    narrow = width // devices
    whole_rows = lax.all_to_all(values.T, "seq", split_axis=0, concat_axis=1, tiled=True)
    total_rows = whole_rows.shape[1]
    own_taps = lax.dynamic_slice_in_dim(whole_filter, lax.axis_index("seq") * narrow, narrow, 1).T
    used_taps = min(own_taps.shape[1], total_rows)
    own_taps = own_taps[:, :used_taps]
    taps_rows = jnp.concatenate(
        [own_taps, jnp.zeros((narrow, total_rows - used_taps), jnp.float32)], axis=1
    )
    row_tables = transform_tables(2 * total_rows)
    spectrum = product(forward_rows(whole_rows, row_tables), forward_rows(taps_rows, row_tables))
    convolved_rows = inverse_rows(spectrum, row_tables)[:, :total_rows]
    convolved = lax.all_to_all(convolved_rows, "seq", split_axis=1, concat_axis=0, tiled=True).T
    hidden = (gates * (convolved + skip[None, :] * values)).astype(jnp.bfloat16)
    return jnp.dot(
        lax.all_gather(hidden, "ch", axis=1, tiled=True),
        out_weight,
        preferred_element_type=jnp.float32,
    )


def toeplitz_kernel(
    tap_sources,
    values_ref,
    gates_ref,
    taps_ref,
    skip_ref,
    weight_ref,
    out_ref,
    x_out,
    h_out,
    x_in,
    h_in,
    x_rows,
    toeplitz,
    h_blocks,
    y_blocks,
    y_out,
    y_in,
    hidden,
    weight,
    weight_sem,
    x_send,
    x_recv,
    h_send,
    h_recv,
    y_send,
    y_recv,
    g_send,
    g_recv,
):
    seq_size, narrow, block_rows = x_out.shape
    tap_rows = h_out.shape[2]
    ch_size, _, width = hidden.shape
    blocks = x_rows.shape[0] // narrow
    per = block_rows // LANES
    groups = narrow // TILE
    me, lane_group = lax.axis_index("seq"), lax.axis_index("ch")
    f32, bf16 = jnp.float32, jnp.bfloat16

    weight_copy = pltpu.make_async_copy(weight_ref, weight, weight_sem)
    weight_copy.start()

    barrier = pltpu.get_barrier_semaphore()
    for step in range(1, seq_size):
        pl.semaphore_signal(
            barrier, inc=1, device_id={"seq": lax.rem(me + step, seq_size)}, device_id_type=MESH
        )
    for step in range(1, ch_size):
        pl.semaphore_signal(
            barrier, inc=1, device_id={"ch": lax.rem(lane_group + step, ch_size)}, device_id_type=MESH
        )

    x_out[...] = values_ref[...].T.astype(bf16).reshape(x_out.shape)

    @pl.when(me < tap_sources)
    def _():
        h_out[...] = taps_ref[...].T.astype(bf16).reshape(h_out.shape)

    h_blocks[...] = jnp.zeros_like(h_blocks)
    pl.semaphore_wait(barrier, seq_size + ch_size - 2)

    x_copies = []
    for step in range(1, seq_size):
        to = lax.rem(me + step, seq_size)
        copy = pltpu.make_async_remote_copy(
            x_out.at[to], x_in.at[me], x_send.at[step], x_recv.at[step],
            device_id={"seq": to}, device_id_type=MESH,
        )
        copy.start()
        x_copies.append(copy)

    def tap_copy(step):
        to = lax.rem(me + step, seq_size)
        return pltpu.make_async_remote_copy(
            h_out.at[to], h_in.at[me], h_send.at[step], h_recv.at[me],
            device_id={"seq": to}, device_id_type=MESH,
        )

    @pl.when(me < tap_sources)
    def _():
        for step in range(1, seq_size):
            tap_copy(step).start()
        h_in[me] = h_out[me]

    x_in[me] = x_out[me]
    for copy in x_copies:
        copy.wait_recv()
    for source in range(seq_size):
        for piece in range(per):
            x_rows[pl.ds(source * per + piece, narrow, stride=blocks), :] = x_in[
                source, :, piece * LANES : (piece + 1) * LANES
            ].astype(f32)

    row_ids = lax.broadcasted_iota(jnp.int32, (LANES, LANES), 0)
    col_ids = lax.broadcasted_iota(jnp.int32, (LANES, LANES), 1)

    def build(channel, carry):
        before = jnp.zeros((LANES, LANES), f32)
        rows = x_rows[pl.ds(pl.multiple_of(channel * blocks, blocks), blocks), :]
        for block in range(blocks):
            row = rows[block : block + 1]
            turned = pltpu.roll(
                jnp.broadcast_to(row, (LANES, LANES)), 0, 1, stride=1, stride_axis=0
            )
            toeplitz[channel, block * LANES : (block + 1) * LANES, :] = jnp.where(
                col_ids >= row_ids, turned, before
            ).astype(bf16)
            before = turned
        return carry

    lax.fori_loop(0, narrow, build, 0)

    for source in range(tap_sources):
        @pl.when(me != source)
        def _():
            pltpu.make_async_remote_copy(
                h_out.at[0], h_in.at[source], h_send.at[0], h_recv.at[source],
                device_id={"seq": source}, device_id_type=MESH,
            ).wait_recv()

    pieces = tap_rows // LANES
    flat_blocks = h_blocks.reshape(narrow * 2 * blocks, LANES)
    for source in range(tap_sources):
        for piece in range(pieces):
            flat_blocks[pl.ds(blocks + source * pieces + piece, narrow, stride=2 * blocks), :] = h_in[
                source, :, piece * LANES : (piece + 1) * LANES
            ].astype(f32)

    def convolve(channel, carry):
        left = jnp.concatenate(
            [h_blocks[channel, blocks - lag : 2 * blocks - lag, :] for lag in range(blocks)], axis=1
        ).astype(bf16)
        y_blocks[pl.ds(pl.multiple_of(channel * blocks, blocks), blocks), :] = jnp.dot(
            left, toeplitz[channel], preferred_element_type=f32
        )
        return carry

    y_copies = []
    for group in range(groups):
        lax.fori_loop(group * TILE, (group + 1) * TILE, convolve, 0)
        rows = slice(group * TILE, (group + 1) * TILE)
        for block in range(blocks):
            y_out[block // per, rows, (block % per) * LANES : (block % per + 1) * LANES] = y_blocks[
                pl.ds(group * TILE * blocks + block, TILE, stride=blocks), :
            ].astype(bf16)
        for step in range(1, seq_size):
            to = lax.rem(me + step, seq_size)
            copy = pltpu.make_async_remote_copy(
                y_out.at[to, rows], y_in.at[me, rows], y_send.at[group, step], y_recv.at[group, step],
                device_id={"seq": to}, device_id_type=MESH,
            )
            copy.start()
            y_copies.append(copy)
    y_in[me] = y_out[me]
    for copy in y_copies:
        copy.wait_recv()

    convolved = y_in[...].astype(f32).reshape(width, block_rows).T
    gated = (gates_ref[...] * (convolved + skip_ref[...] * values_ref[...])).astype(bf16)
    hidden[lane_group] = gated

    g_copies = []
    for step in range(1, ch_size):
        copy = pltpu.make_async_remote_copy(
            hidden.at[lane_group], hidden.at[lane_group], g_send.at[step], g_recv.at[step],
            device_id={"ch": lax.rem(lane_group + step, ch_size)}, device_id_type=MESH,
        )
        copy.start()
        g_copies.append(copy)
    weight_copy.wait()
    out_ref[...] = jnp.dot(gated, weight[lane_group], preferred_element_type=f32)
    for step in range(1, ch_size):
        source = lax.rem(lane_group + ch_size - step, ch_size)
        g_copies[step - 1].wait_recv()
        out_ref[...] += jnp.dot(hidden[source], weight[source], preferred_element_type=f32)

    for copy in x_copies + y_copies + g_copies:
        copy.wait_send()

    @pl.when(me < tap_sources)
    def _():
        for step in range(1, seq_size):
            tap_copy(step).wait_send()


def toeplitz_body(values, gates, filter_taps, skip, out_weight):
    seq_size, ch_size = lax.axis_size("seq"), lax.axis_size("ch")
    block_rows, width = values.shape
    tap_rows = filter_taps.shape[0]
    narrow = width // seq_size
    total = block_rows * seq_size
    sources = min(tap_rows * seq_size, total) // tap_rows
    columns = out_weight.shape[1]
    f32, bf16 = jnp.float32, jnp.bfloat16
    vmem = pl.BlockSpec(memory_space=pltpu.VMEM)
    dma = pltpu.SemaphoreType.DMA
    return pl.pallas_call(
        functools.partial(toeplitz_kernel, sources),
        out_shape=jax.ShapeDtypeStruct((block_rows, columns), f32),
        in_specs=[vmem] * 4 + [pl.BlockSpec(memory_space=pl.ANY)],
        out_specs=vmem,
        scratch_shapes=[
            pltpu.VMEM((seq_size, narrow, block_rows), bf16),
            pltpu.VMEM((seq_size, narrow, tap_rows), bf16),
            pltpu.VMEM((seq_size, narrow, block_rows), bf16),
            pltpu.VMEM((sources, narrow, tap_rows), bf16),
            pltpu.VMEM((narrow * (total // LANES), LANES), f32),
            pltpu.VMEM((narrow, total, LANES), bf16),
            pltpu.VMEM((narrow, 2 * (total // LANES), LANES), f32),
            pltpu.VMEM((narrow * (total // LANES), LANES), f32),
            pltpu.VMEM((seq_size, narrow, block_rows), bf16),
            pltpu.VMEM((seq_size, narrow, block_rows), bf16),
            pltpu.VMEM((ch_size, block_rows, width), bf16),
            pltpu.VMEM((ch_size, width, columns), bf16),
            dma(()),
            dma((seq_size,)),
            dma((seq_size,)),
            dma((seq_size,)),
            dma((sources,)),
            dma((narrow // TILE, seq_size)),
            dma((narrow // TILE, seq_size)),
            dma((ch_size,)),
            dma((ch_size,)),
        ],
        compiler_params=pltpu.CompilerParams(
            collective_id=0, has_side_effects=True, vmem_limit_bytes=48 * 1024 * 1024
        ),
    )(
        values,
        gates,
        filter_taps,
        skip.reshape(1, width),
        out_weight.reshape(ch_size, width, columns),
    )


def local_body(values, gates, filter_taps, skip, out_weight):
    seq_size = lax.axis_size("seq")
    block_rows, width = values.shape
    tap_rows = filter_taps.shape[0]
    narrow = width // seq_size
    total = block_rows * seq_size
    fits = (
        width % (seq_size * TILE) == 0
        and width % LANES == 0
        and block_rows % LANES == 0
        and total // LANES % 8 == 0
        and tap_rows % LANES == 0
        and total % tap_rows == 0
        and narrow * total * LANES * 2 <= 32 * 1024 * 1024
    )
    chosen = toeplitz_body if fits else body
    return chosen(values, gates, filter_taps, skip, out_weight)


def solution(mesh):
    placed = (P("seq", "ch"), P("seq", "ch"), P("seq", "ch"), P("ch"), P(None, "ch"))
    return jax.shard_map(
        local_body, mesh=mesh, in_specs=placed, out_specs=P("seq", "ch"), check_vma=False
    )
```

```python
import functools
import math

import jax
import jax.numpy as jnp
from jax import lax
from jax.experimental import pallas as pl
from jax.experimental.pallas import tpu as pltpu
from jax.sharding import PartitionSpec as P

HIGHEST = lax.Precision.HIGHEST
MESH = pl.DeviceIdType.MESH
LANES = 128
TILE = 16
BUILD_UNROLL = 2
CONV_UNROLL = 4


def split_length(length):
    leading = 1
    for factor in range(1, math.isqrt(length) + 1):
        if length % factor == 0:
            leading = factor
    return (leading, length // leading)


def phase_table(count_rows, count_cols, modulus):
    row_ids = jnp.arange(count_rows, dtype=jnp.int32)
    col_ids = jnp.arange(count_cols, dtype=jnp.int32)
    wrapped = row_ids[:, None] * col_ids[None, :] % modulus
    phases = 2.0 * math.pi / modulus * wrapped.astype(jnp.float32)
    return (jnp.cos(phases), jnp.sin(phases))


def complex_form(cosine, sine):
    upper = jnp.stack([cosine, -sine], axis=1)
    lower = jnp.stack([sine, cosine], axis=1)
    return jnp.stack([upper, lower], axis=0)


def transform_tables(length):
    rows_lead, rows_tail = split_length(length)
    cos_lead, sin_lead = phase_table(rows_lead, rows_lead, rows_lead)
    cos_tail, sin_tail = phase_table(rows_tail, rows_tail, rows_tail)
    cos_twist, sin_twist = phase_table(rows_lead, rows_tail, length)
    lead_table = jnp.stack([cos_lead, -sin_lead])
    tail_forward = complex_form(cos_tail, -sin_tail)
    tail_inverse = complex_form(cos_tail, sin_tail)
    return (
        lead_table,
        tail_forward,
        tail_inverse,
        cos_twist,
        sin_twist,
        rows_lead,
        rows_tail,
        length,
    )


def twist_rows(section, cosine, sine):
    real_part = section[0] * cosine[None] - section[1] * sine[None]
    imag_part = section[0] * sine[None] + section[1] * cosine[None]
    return jnp.stack([real_part, imag_part])


def forward_rows(rows, tables):
    lead_table, tail_forward, tail_inverse, cos_twist, sin_twist, rows_lead, rows_tail, length = (
        tables
    )
    signal = jnp.concatenate([rows, jnp.zeros_like(rows)], axis=1).reshape(
        rows.shape[0], rows_lead, rows_tail
    )
    section = jnp.einsum("pft,cts->pcfs", lead_table, signal, precision=HIGHEST)
    twisted = twist_rows(section, cos_twist, -sin_twist)
    return jnp.einsum("pgrs,rcfs->pcfg", tail_forward, twisted, precision=HIGHEST)


def inverse_rows(spectrum, tables):
    lead_table, tail_forward, tail_inverse, cos_twist, sin_twist, rows_lead, rows_tail, length = (
        tables
    )
    section = jnp.einsum("pgrs,rcfs->pcfg", tail_inverse, spectrum, precision=HIGHEST)
    twisted = twist_rows(section, cos_twist, sin_twist)
    signal = jnp.einsum("rft,rcfs->cts", lead_table, twisted, precision=HIGHEST) / length
    return signal.reshape(signal.shape[0], length)


def product(left, right):
    real_part = left[0] * right[0] - left[1] * right[1]
    imag_part = left[0] * right[1] + left[1] * right[0]
    return jnp.stack([real_part, imag_part])


def body(values, gates, filter_taps, skip, out_weight):
    block_rows, width = values.shape
    whole_filter = lax.all_gather(filter_taps, "seq", axis=0, tiled=True)
    devices = lax.axis_size("seq")
    narrow = width // devices
    whole_rows = lax.all_to_all(values.T, "seq", split_axis=0, concat_axis=1, tiled=True)
    total_rows = whole_rows.shape[1]
    own_taps = lax.dynamic_slice_in_dim(whole_filter, lax.axis_index("seq") * narrow, narrow, 1).T
    used_taps = min(own_taps.shape[1], total_rows)
    own_taps = own_taps[:, :used_taps]
    taps_rows = jnp.concatenate(
        [own_taps, jnp.zeros((narrow, total_rows - used_taps), jnp.float32)], axis=1
    )
    row_tables = transform_tables(2 * total_rows)
    spectrum = product(forward_rows(whole_rows, row_tables), forward_rows(taps_rows, row_tables))
    convolved_rows = inverse_rows(spectrum, row_tables)[:, :total_rows]
    convolved = lax.all_to_all(convolved_rows, "seq", split_axis=1, concat_axis=0, tiled=True).T
    hidden = (gates * (convolved + skip[None, :] * values)).astype(jnp.bfloat16)
    return jnp.dot(
        lax.all_gather(hidden, "ch", axis=1, tiled=True),
        out_weight,
        preferred_element_type=jnp.float32,
    )


def toeplitz_kernel(
    tap_sources,
    values_hbm,
    gates_hbm,
    taps_hbm,
    skip_ref,
    weight_hbm,
    out_hbm,
    values_ref,
    gates_ref,
    taps_ref,
    out_ref,
    x_out,
    h_out,
    x_in,
    h_in,
    x_rows,
    toeplitz,
    h_blocks,
    y_blocks,
    y_out,
    y_in,
    hidden,
    weight,
    load_sem,
    out_sem,
    x_send,
    x_recv,
    h_send,
    h_recv,
    y_send,
    y_recv,
    g_send,
    g_recv,
):
    seq_size, narrow, block_rows = x_out.shape
    tap_rows = h_out.shape[2]
    ch_size, _, width = hidden.shape
    blocks = x_rows.shape[0] // narrow
    per = block_rows // LANES
    groups = narrow // TILE
    me, lane_group = lax.axis_index("seq"), lax.axis_index("ch")
    f32, bf16 = jnp.float32, jnp.bfloat16

    loads = [
        pltpu.make_async_copy(source, target, load_sem.at[place])
        for place, (source, target) in enumerate(
            (
                (values_hbm, values_ref),
                (taps_hbm, taps_ref),
                (gates_hbm, gates_ref),
                (weight_hbm, weight),
            )
        )
    ]
    for load in loads:
        load.start()

    barrier = pltpu.get_barrier_semaphore()
    for step in range(1, seq_size):
        pl.semaphore_signal(
            barrier, inc=1, device_id={"seq": lax.rem(me + step, seq_size)}, device_id_type=MESH
        )
    for step in range(1, ch_size):
        pl.semaphore_signal(
            barrier, inc=1, device_id={"ch": lax.rem(lane_group + step, ch_size)}, device_id_type=MESH
        )

    h_blocks[...] = jnp.zeros_like(h_blocks)
    loads[0].wait()
    x_out[...] = values_ref[...].T.astype(bf16).reshape(x_out.shape)
    pl.semaphore_wait(barrier, seq_size + ch_size - 2)

    x_copies = []
    for step in range(1, seq_size):
        to = lax.rem(me + step, seq_size)
        copy = pltpu.make_async_remote_copy(
            x_out.at[to], x_in.at[me], x_send.at[step], x_recv.at[step],
            device_id={"seq": to}, device_id_type=MESH,
        )
        copy.start()
        x_copies.append(copy)

    loads[1].wait()

    def tap_copy(step):
        to = lax.rem(me + step, seq_size)
        return pltpu.make_async_remote_copy(
            h_out.at[to], h_in.at[me], h_send.at[step], h_recv.at[me],
            device_id={"seq": to}, device_id_type=MESH,
        )

    @pl.when(me < tap_sources)
    def _():
        h_out[...] = taps_ref[...].T.astype(bf16).reshape(h_out.shape)
        for step in range(1, seq_size):
            tap_copy(step).start()
        h_in[me] = h_out[me]

    x_in[me] = x_out[me]
    for copy in x_copies:
        copy.wait_recv()
    for source in range(seq_size):
        for piece in range(per):
            x_rows[pl.ds(source * per + piece, narrow, stride=blocks), :] = x_in[
                source, :, piece * LANES : (piece + 1) * LANES
            ].astype(f32)

    row_ids = lax.broadcasted_iota(jnp.int32, (LANES, LANES), 0)
    col_ids = lax.broadcasted_iota(jnp.int32, (LANES, LANES), 1)

    def build_one(channel):
        before = jnp.zeros((LANES, LANES), f32)
        rows = x_rows[pl.ds(pl.multiple_of(channel * blocks, blocks), blocks), :]
        for block in range(blocks):
            row = rows[block : block + 1]
            turned = pltpu.roll(
                jnp.broadcast_to(row, (LANES, LANES)), 0, 1, stride=1, stride_axis=0
            )
            toeplitz[channel, block * LANES : (block + 1) * LANES, :] = jnp.where(
                col_ids >= row_ids, turned, before
            ).astype(bf16)
            before = turned

    def build(turn, carry):
        for part in range(BUILD_UNROLL):
            build_one(turn * BUILD_UNROLL + part)
        return carry

    lax.fori_loop(0, narrow // BUILD_UNROLL, build, 0)

    for source in range(tap_sources):
        @pl.when(me != source)
        def _():
            pltpu.make_async_remote_copy(
                h_out.at[0], h_in.at[source], h_send.at[0], h_recv.at[source],
                device_id={"seq": source}, device_id_type=MESH,
            ).wait_recv()

    pieces = tap_rows // LANES
    flat_blocks = h_blocks.reshape(narrow * 2 * blocks, LANES)
    for source in range(tap_sources):
        for piece in range(pieces):
            flat_blocks[pl.ds(blocks + source * pieces + piece, narrow, stride=2 * blocks), :] = h_in[
                source, :, piece * LANES : (piece + 1) * LANES
            ].astype(f32)

    def convolve_one(channel):
        left = jnp.concatenate(
            [h_blocks[channel, blocks - lag : 2 * blocks - lag, :] for lag in range(blocks)], axis=1
        ).astype(bf16)
        y_blocks[pl.ds(pl.multiple_of(channel * blocks, blocks), blocks), :] = jnp.dot(
            left, toeplitz[channel], preferred_element_type=f32
        )

    def convolve(turn, carry):
        for part in range(CONV_UNROLL):
            convolve_one(turn * CONV_UNROLL + part)
        return carry

    y_copies = []
    for group in range(groups):
        turns = TILE // CONV_UNROLL
        lax.fori_loop(group * turns, (group + 1) * turns, convolve, 0)
        rows = slice(group * TILE, (group + 1) * TILE)
        for block in range(blocks):
            y_out[block // per, rows, (block % per) * LANES : (block % per + 1) * LANES] = y_blocks[
                pl.ds(group * TILE * blocks + block, TILE, stride=blocks), :
            ].astype(bf16)
        for step in range(1, seq_size):
            to = lax.rem(me + step, seq_size)
            copy = pltpu.make_async_remote_copy(
                y_out.at[to, rows], y_in.at[me, rows], y_send.at[group, step], y_recv.at[group, step],
                device_id={"seq": to}, device_id_type=MESH,
            )
            copy.start()
            y_copies.append(copy)
    y_in[me] = y_out[me]
    for copy in y_copies:
        copy.wait_recv()

    partner = lane_group + 1 - 2 * lax.rem(lane_group, 2)
    pairs = ch_size // 2

    def spread(kind, piece, slot, to):
        block = hidden.at[slot, pl.ds(piece * LANES, LANES)]
        copy = pltpu.make_async_remote_copy(
            block, block, g_send.at[kind, piece], g_recv.at[kind, piece],
            device_id={"ch": to}, device_id_type=MESH,
        )
        copy.start()
        g_copies.append(copy)
        return copy

    def add_product(piece, slot, first=False):
        rows = slice(piece * LANES, (piece + 1) * LANES)
        term = jnp.dot(hidden[slot, rows], weight[slot], preferred_element_type=f32)
        out_ref[rows] = term if first else out_ref[rows] + term

    g_copies, direct, relayed = [], {}, {}
    loads[2].wait()
    for piece in range(per):
        rows = slice(piece * LANES, (piece + 1) * LANES)
        convolved = y_in[:, :, rows].astype(f32).reshape(width, LANES).T
        hidden[lane_group, rows] = (
            gates_ref[rows] * (convolved + skip_ref[...] * values_ref[rows])
        ).astype(bf16)
        for pair in range(1, pairs):
            direct[pair, piece] = spread(
                2 * pair - 1, piece, lane_group, lax.rem(lane_group + 2 * pair, ch_size)
            )
        direct[0, piece] = spread(0, piece, lane_group, partner)
    loads[3].wait()
    for piece in range(per):
        add_product(piece, lane_group, True)
    for piece in range(per):
        direct[0, piece].wait_recv()
        add_product(piece, partner)
    for piece in range(per):
        for pair in range(1, pairs):
            slot = lax.rem(lane_group + ch_size - 2 * pair, ch_size)
            direct[pair, piece].wait_recv()
            relayed[pair, piece] = spread(2 * pair, piece, slot, partner)
            add_product(piece, slot)
    stores = []
    for piece in range(per):
        rows = pl.ds(piece * LANES, LANES)
        for pair in range(1, pairs):
            slot = lax.rem(partner + ch_size - 2 * pair, ch_size)
            relayed[pair, piece].wait_recv()
            add_product(piece, slot)
        store = pltpu.make_async_copy(out_ref.at[rows], out_hbm.at[rows], out_sem.at[piece])
        store.start()
        stores.append(store)
    for store in stores:
        store.wait()

    for copy in x_copies + y_copies + g_copies:
        copy.wait_send()

    @pl.when(me < tap_sources)
    def _():
        for step in range(1, seq_size):
            tap_copy(step).wait_send()


def toeplitz_body(values, gates, filter_taps, skip, out_weight):
    seq_size, ch_size = lax.axis_size("seq"), lax.axis_size("ch")
    block_rows, width = values.shape
    tap_rows = filter_taps.shape[0]
    narrow = width // seq_size
    total = block_rows * seq_size
    sources = min(tap_rows * seq_size, total) // tap_rows
    columns = out_weight.shape[1]
    f32, bf16 = jnp.float32, jnp.bfloat16
    vmem = pl.BlockSpec(memory_space=pltpu.VMEM)
    hbm = pl.BlockSpec(memory_space=pl.ANY)
    per = block_rows // LANES
    dma = pltpu.SemaphoreType.DMA
    return pl.pallas_call(
        functools.partial(toeplitz_kernel, sources),
        out_shape=jax.ShapeDtypeStruct((block_rows, columns), f32),
        in_specs=[hbm] * 3 + [vmem, hbm],
        out_specs=hbm,
        scratch_shapes=[
            pltpu.VMEM((block_rows, width), f32),
            pltpu.VMEM((block_rows, width), f32),
            pltpu.VMEM((tap_rows, width), f32),
            pltpu.VMEM((block_rows, columns), f32),
            pltpu.VMEM((seq_size, narrow, block_rows), bf16),
            pltpu.VMEM((seq_size, narrow, tap_rows), bf16),
            pltpu.VMEM((seq_size, narrow, block_rows), bf16),
            pltpu.VMEM((sources, narrow, tap_rows), bf16),
            pltpu.VMEM((narrow * (total // LANES), LANES), f32),
            pltpu.VMEM((narrow, total, LANES), bf16),
            pltpu.VMEM((narrow, 2 * (total // LANES), LANES), f32),
            pltpu.VMEM((narrow * (total // LANES), LANES), f32),
            pltpu.VMEM((seq_size, narrow, block_rows), bf16),
            pltpu.VMEM((seq_size, narrow, block_rows), bf16),
            pltpu.VMEM((ch_size, block_rows, width), bf16),
            pltpu.VMEM((ch_size, width, columns), bf16),
            dma((4,)),
            dma((per,)),
            dma((seq_size,)),
            dma((seq_size,)),
            dma((seq_size,)),
            dma((sources,)),
            dma((narrow // TILE, seq_size)),
            dma((narrow // TILE, seq_size)),
            dma((ch_size, per)),
            dma((ch_size, per)),
        ],
        compiler_params=pltpu.CompilerParams(
            collective_id=0, has_side_effects=True, vmem_limit_bytes=63000 * 1024
        ),
    )(
        values,
        gates,
        filter_taps,
        skip.reshape(1, width),
        out_weight.reshape(ch_size, width, columns),
    )


def local_body(values, gates, filter_taps, skip, out_weight):
    seq_size = lax.axis_size("seq")
    block_rows, width = values.shape
    tap_rows = filter_taps.shape[0]
    narrow = width // seq_size
    total = block_rows * seq_size
    fits = (
        width % (seq_size * TILE) == 0
        and lax.axis_size("ch") % 2 == 0
        and width % LANES == 0
        and block_rows % LANES == 0
        and total // LANES % 8 == 0
        and tap_rows % LANES == 0
        and total % tap_rows == 0
        and narrow * total * LANES * 2 <= 32 * 1024 * 1024
    )
    chosen = toeplitz_body if fits else body
    return chosen(values, gates, filter_taps, skip, out_weight)


def solution(mesh):
    placed = (P("seq", "ch"), P("seq", "ch"), P("seq", "ch"), P("ch"), P(None, "ch"))
    return jax.shard_map(
        local_body, mesh=mesh, in_specs=placed, out_specs=P("seq", "ch"), check_vma=False
    )
```

```python
import functools
import math

import jax
import jax.numpy as jnp
from jax import lax
from jax.experimental import pallas as pl
from jax.experimental.pallas import tpu as pltpu
from jax.sharding import PartitionSpec as P

HIGHEST = lax.Precision.HIGHEST
MESH = pl.DeviceIdType.MESH
LANES = 128
TILE = 16
BUILD_UNROLL = 8
CONV_UNROLL = 16


def split_length(length):
    leading = 1
    for factor in range(1, math.isqrt(length) + 1):
        if length % factor == 0:
            leading = factor
    return (leading, length // leading)


def phase_table(count_rows, count_cols, modulus):
    row_ids = jnp.arange(count_rows, dtype=jnp.int32)
    col_ids = jnp.arange(count_cols, dtype=jnp.int32)
    wrapped = row_ids[:, None] * col_ids[None, :] % modulus
    phases = 2.0 * math.pi / modulus * wrapped.astype(jnp.float32)
    return (jnp.cos(phases), jnp.sin(phases))


def complex_form(cosine, sine):
    upper = jnp.stack([cosine, -sine], axis=1)
    lower = jnp.stack([sine, cosine], axis=1)
    return jnp.stack([upper, lower], axis=0)


def transform_tables(length):
    rows_lead, rows_tail = split_length(length)
    cos_lead, sin_lead = phase_table(rows_lead, rows_lead, rows_lead)
    cos_tail, sin_tail = phase_table(rows_tail, rows_tail, rows_tail)
    cos_twist, sin_twist = phase_table(rows_lead, rows_tail, length)
    lead_table = jnp.stack([cos_lead, -sin_lead])
    tail_forward = complex_form(cos_tail, -sin_tail)
    tail_inverse = complex_form(cos_tail, sin_tail)
    return (
        lead_table,
        tail_forward,
        tail_inverse,
        cos_twist,
        sin_twist,
        rows_lead,
        rows_tail,
        length,
    )


def twist_rows(section, cosine, sine):
    real_part = section[0] * cosine[None] - section[1] * sine[None]
    imag_part = section[0] * sine[None] + section[1] * cosine[None]
    return jnp.stack([real_part, imag_part])


def forward_rows(rows, tables):
    lead_table, tail_forward, tail_inverse, cos_twist, sin_twist, rows_lead, rows_tail, length = (
        tables
    )
    signal = jnp.concatenate([rows, jnp.zeros_like(rows)], axis=1).reshape(
        rows.shape[0], rows_lead, rows_tail
    )
    section = jnp.einsum("pft,cts->pcfs", lead_table, signal, precision=HIGHEST)
    twisted = twist_rows(section, cos_twist, -sin_twist)
    return jnp.einsum("pgrs,rcfs->pcfg", tail_forward, twisted, precision=HIGHEST)


def inverse_rows(spectrum, tables):
    lead_table, tail_forward, tail_inverse, cos_twist, sin_twist, rows_lead, rows_tail, length = (
        tables
    )
    section = jnp.einsum("pgrs,rcfs->pcfg", tail_inverse, spectrum, precision=HIGHEST)
    twisted = twist_rows(section, cos_twist, sin_twist)
    signal = jnp.einsum("rft,rcfs->cts", lead_table, twisted, precision=HIGHEST) / length
    return signal.reshape(signal.shape[0], length)


def product(left, right):
    real_part = left[0] * right[0] - left[1] * right[1]
    imag_part = left[0] * right[1] + left[1] * right[0]
    return jnp.stack([real_part, imag_part])


def body(values, gates, filter_taps, skip, out_weight):
    block_rows, width = values.shape
    whole_filter = lax.all_gather(filter_taps, "seq", axis=0, tiled=True)
    devices = lax.axis_size("seq")
    narrow = width // devices
    whole_rows = lax.all_to_all(values.T, "seq", split_axis=0, concat_axis=1, tiled=True)
    total_rows = whole_rows.shape[1]
    own_taps = lax.dynamic_slice_in_dim(whole_filter, lax.axis_index("seq") * narrow, narrow, 1).T
    used_taps = min(own_taps.shape[1], total_rows)
    own_taps = own_taps[:, :used_taps]
    taps_rows = jnp.concatenate(
        [own_taps, jnp.zeros((narrow, total_rows - used_taps), jnp.float32)], axis=1
    )
    row_tables = transform_tables(2 * total_rows)
    spectrum = product(forward_rows(whole_rows, row_tables), forward_rows(taps_rows, row_tables))
    convolved_rows = inverse_rows(spectrum, row_tables)[:, :total_rows]
    convolved = lax.all_to_all(convolved_rows, "seq", split_axis=1, concat_axis=0, tiled=True).T
    hidden = (gates * (convolved + skip[None, :] * values)).astype(jnp.bfloat16)
    return jnp.dot(
        lax.all_gather(hidden, "ch", axis=1, tiled=True),
        out_weight,
        preferred_element_type=jnp.float32,
    )


def toeplitz_kernel(
    tap_sources,
    values_hbm,
    gates_hbm,
    taps_hbm,
    skip_ref,
    weight_hbm,
    out_hbm,
    values_ref,
    gates_ref,
    taps_ref,
    out_ref,
    x_out,
    h_out,
    x_in,
    h_in,
    x_rows,
    toeplitz,
    h_blocks,
    y_blocks,
    y_out,
    y_in,
    hidden,
    weight,
    load_sem,
    out_sem,
    x_send,
    x_recv,
    h_send,
    h_recv,
    y_send,
    y_recv,
    g_send,
    g_recv,
):
    seq_size, narrow, block_rows = x_out.shape
    tap_rows = h_out.shape[2]
    ch_size, _, width = hidden.shape
    blocks = x_rows.shape[0] // narrow
    per = block_rows // LANES
    me, lane_group = lax.axis_index("seq"), lax.axis_index("ch")
    f32, bf16 = jnp.float32, jnp.bfloat16

    loads = [
        pltpu.make_async_copy(source, target, load_sem.at[place])
        for place, (source, target) in enumerate(
            (
                (values_hbm, values_ref),
                (taps_hbm, taps_ref),
                (gates_hbm, gates_ref),
                (weight_hbm, weight),
            )
        )
    ]
    for load in loads:
        load.start()

    barrier = pltpu.get_barrier_semaphore()
    for step in range(1, seq_size):
        pl.semaphore_signal(
            barrier, inc=1, device_id={"seq": lax.rem(me + step, seq_size)}, device_id_type=MESH
        )
    for step in range(1, ch_size):
        pl.semaphore_signal(
            barrier, inc=1, device_id={"ch": lax.rem(lane_group + step, ch_size)}, device_id_type=MESH
        )

    h_blocks[...] = jnp.zeros_like(h_blocks)
    loads[0].wait()
    x_out[...] = values_ref[...].T.astype(bf16).reshape(x_out.shape)
    pl.semaphore_wait(barrier, seq_size + ch_size - 2)

    groups = narrow // TILE
    x_copies = []
    for group in range(groups):
        part = pl.ds(group * TILE, TILE)
        for step in range(1, seq_size):
            to = lax.rem(me + step, seq_size)
            copy = pltpu.make_async_remote_copy(
                x_out.at[to, part], x_in.at[me, part],
                x_send.at[group, step], x_recv.at[group, step],
                device_id={"seq": to}, device_id_type=MESH,
            )
            copy.start()
            x_copies.append(copy)

    loads[1].wait()

    def tap_copy(step):
        to = lax.rem(me + step, seq_size)
        return pltpu.make_async_remote_copy(
            h_out.at[to], h_in.at[me], h_send.at[step], h_recv.at[me],
            device_id={"seq": to}, device_id_type=MESH,
        )

    @pl.when(me < tap_sources)
    def _():
        h_out[...] = taps_ref[...].T.astype(bf16).reshape(h_out.shape)
        for step in range(1, seq_size):
            tap_copy(step).start()
        h_in[me] = h_out[me]

    x_in[me] = x_out[me]
    row_ids = lax.broadcasted_iota(jnp.int32, (LANES, LANES), 0)
    col_ids = lax.broadcasted_iota(jnp.int32, (LANES, LANES), 1)

    def build_one(channel):
        before = jnp.zeros((LANES, LANES), f32)
        rows = x_rows[pl.ds(pl.multiple_of(channel * blocks, blocks), blocks), :]
        for block in range(blocks):
            row = rows[block : block + 1]
            turned = pltpu.roll(
                jnp.broadcast_to(row, (LANES, LANES)), 0, 1, stride=1, stride_axis=0
            )
            toeplitz[channel, block * LANES : (block + 1) * LANES, :] = jnp.where(
                col_ids >= row_ids, turned, before
            ).astype(bf16)
            before = turned

    def build(turn, carry):
        for part in range(BUILD_UNROLL):
            build_one(turn * BUILD_UNROLL + part)
        return carry

    turns = TILE // BUILD_UNROLL
    for group in range(groups):
        for copy in x_copies[group * (seq_size - 1) : (group + 1) * (seq_size - 1)]:
            copy.wait_recv()
        for source in range(seq_size):
            for piece in range(per):
                x_rows[pl.ds(group * TILE * blocks + source * per + piece, TILE, stride=blocks), :] = x_in[
                    source, group * TILE : (group + 1) * TILE, piece * LANES : (piece + 1) * LANES
                ].astype(f32)
        lax.fori_loop(group * turns, (group + 1) * turns, build, 0)

    for source in range(tap_sources):
        @pl.when(me != source)
        def _():
            pltpu.make_async_remote_copy(
                h_out.at[0], h_in.at[source], h_send.at[0], h_recv.at[source],
                device_id={"seq": source}, device_id_type=MESH,
            ).wait_recv()

    pieces = tap_rows // LANES
    flat_blocks = h_blocks.reshape(narrow * 2 * blocks, LANES)
    for source in range(tap_sources):
        for piece in range(pieces):
            flat_blocks[pl.ds(blocks + source * pieces + piece, narrow, stride=2 * blocks), :] = h_in[
                source, :, piece * LANES : (piece + 1) * LANES
            ].astype(f32)

    def convolve_one(channel):
        left = jnp.concatenate(
            [h_blocks[channel, blocks - lag : 2 * blocks - lag, :] for lag in range(blocks)], axis=1
        ).astype(bf16)
        y_blocks[pl.ds(pl.multiple_of(channel * blocks, blocks), blocks), :] = jnp.dot(
            left, toeplitz[channel], preferred_element_type=f32
        )

    def convolve(turn, carry):
        for part in range(CONV_UNROLL):
            convolve_one(turn * CONV_UNROLL + part)
        return carry

    lax.fori_loop(0, narrow // CONV_UNROLL, convolve, 0)
    for block in range(blocks):
        y_out[block // per, :, (block % per) * LANES : (block % per + 1) * LANES] = y_blocks[
            pl.ds(block, narrow, stride=blocks), :
        ].astype(bf16)
    y_copies = {}
    for piece in range(per):
        span = pl.ds(piece * LANES, LANES)
        for step in range(1, seq_size):
            to = lax.rem(me + step, seq_size)
            y_copies[piece, step] = pltpu.make_async_remote_copy(
                y_out.at[to, :, span], y_in.at[me, :, span],
                y_send.at[piece, step], y_recv.at[piece, step],
                device_id={"seq": to}, device_id_type=MESH,
            )
            y_copies[piece, step].start()
    y_in[me] = y_out[me]

    partner = lane_group + 1 - 2 * lax.rem(lane_group, 2)
    pairs = ch_size // 2

    def spread(kind, piece, slot, to):
        block = hidden.at[slot, pl.ds(piece * LANES, LANES)]
        copy = pltpu.make_async_remote_copy(
            block, block, g_send.at[kind, piece], g_recv.at[kind, piece],
            device_id={"ch": to}, device_id_type=MESH,
        )
        copy.start()
        g_copies.append(copy)
        return copy

    def add_product(piece, slot, first=False):
        rows = slice(piece * LANES, (piece + 1) * LANES)
        term = jnp.dot(hidden[slot, rows], weight[slot], preferred_element_type=f32)
        out_ref[rows] = term if first else out_ref[rows] + term

    g_copies, direct, relayed = [], {}, {}
    loads[2].wait()
    for piece in range(per):
        rows = slice(piece * LANES, (piece + 1) * LANES)
        for step in range(1, seq_size):
            y_copies[piece, step].wait_recv()
        convolved = y_in[:, :, rows].astype(f32).reshape(width, LANES).T
        hidden[lane_group, rows] = (
            gates_ref[rows] * (convolved + skip_ref[...] * values_ref[rows])
        ).astype(bf16)
        for pair in range(1, pairs):
            direct[pair, piece] = spread(
                2 * pair - 1, piece, lane_group, lax.rem(lane_group + 2 * pair, ch_size)
            )
        direct[0, piece] = spread(0, piece, lane_group, partner)
    loads[3].wait()
    for piece in range(per):
        add_product(piece, lane_group, True)
    for piece in range(per):
        direct[0, piece].wait_recv()
        add_product(piece, partner)
    for piece in range(per):
        for pair in range(1, pairs):
            slot = lax.rem(lane_group + ch_size - 2 * pair, ch_size)
            direct[pair, piece].wait_recv()
            relayed[pair, piece] = spread(2 * pair, piece, slot, partner)
            add_product(piece, slot)
    stores = []
    for piece in range(per):
        rows = pl.ds(piece * LANES, LANES)
        for pair in range(1, pairs):
            slot = lax.rem(partner + ch_size - 2 * pair, ch_size)
            relayed[pair, piece].wait_recv()
            add_product(piece, slot)
        store = pltpu.make_async_copy(out_ref.at[rows], out_hbm.at[rows], out_sem.at[piece])
        store.start()
        stores.append(store)
    for store in stores:
        store.wait()

    for copy in x_copies + list(y_copies.values()) + g_copies:
        copy.wait_send()

    @pl.when(me < tap_sources)
    def _():
        for step in range(1, seq_size):
            tap_copy(step).wait_send()


def toeplitz_body(values, gates, filter_taps, skip, out_weight):
    seq_size, ch_size = lax.axis_size("seq"), lax.axis_size("ch")
    block_rows, width = values.shape
    tap_rows = filter_taps.shape[0]
    narrow = width // seq_size
    total = block_rows * seq_size
    sources = min(tap_rows * seq_size, total) // tap_rows
    columns = out_weight.shape[1]
    f32, bf16 = jnp.float32, jnp.bfloat16
    vmem = pl.BlockSpec(memory_space=pltpu.VMEM)
    hbm = pl.BlockSpec(memory_space=pl.ANY)
    per = block_rows // LANES
    dma = pltpu.SemaphoreType.DMA
    return pl.pallas_call(
        functools.partial(toeplitz_kernel, sources),
        out_shape=jax.ShapeDtypeStruct((block_rows, columns), f32),
        in_specs=[hbm] * 3 + [vmem, hbm],
        out_specs=hbm,
        scratch_shapes=[
            pltpu.VMEM((block_rows, width), f32),
            pltpu.VMEM((block_rows, width), f32),
            pltpu.VMEM((tap_rows, width), f32),
            pltpu.VMEM((block_rows, columns), f32),
            pltpu.VMEM((seq_size, narrow, block_rows), bf16),
            pltpu.VMEM((seq_size, narrow, tap_rows), bf16),
            pltpu.VMEM((seq_size, narrow, block_rows), bf16),
            pltpu.VMEM((sources, narrow, tap_rows), bf16),
            pltpu.VMEM((narrow * (total // LANES), LANES), f32),
            pltpu.VMEM((narrow, total, LANES), bf16),
            pltpu.VMEM((narrow, 2 * (total // LANES), LANES), f32),
            pltpu.VMEM((narrow * (total // LANES), LANES), f32),
            pltpu.VMEM((seq_size, narrow, block_rows), bf16),
            pltpu.VMEM((seq_size, narrow, block_rows), bf16),
            pltpu.VMEM((ch_size, block_rows, width), bf16),
            pltpu.VMEM((ch_size, width, columns), bf16),
            dma((4,)),
            dma((per,)),
            dma((narrow // TILE, seq_size)),
            dma((narrow // TILE, seq_size)),
            dma((seq_size,)),
            dma((sources,)),
            dma((per, seq_size)),
            dma((per, seq_size)),
            dma((ch_size, per)),
            dma((ch_size, per)),
        ],
        compiler_params=pltpu.CompilerParams(
            collective_id=0, has_side_effects=True, vmem_limit_bytes=63000 * 1024
        ),
    )(
        values,
        gates,
        filter_taps,
        skip.reshape(1, width),
        out_weight.reshape(ch_size, width, columns),
    )


def local_body(values, gates, filter_taps, skip, out_weight):
    seq_size = lax.axis_size("seq")
    block_rows, width = values.shape
    tap_rows = filter_taps.shape[0]
    narrow = width // seq_size
    total = block_rows * seq_size
    fits = (
        width % (seq_size * TILE) == 0
        and lax.axis_size("ch") % 2 == 0
        and width % LANES == 0
        and block_rows % LANES == 0
        and total // LANES % 8 == 0
        and tap_rows % LANES == 0
        and total % tap_rows == 0
        and narrow * total * LANES * 2 <= 32 * 1024 * 1024
    )
    chosen = toeplitz_body if fits else body
    return chosen(values, gates, filter_taps, skip, out_weight)


def solution(mesh):
    placed = (P("seq", "ch"), P("seq", "ch"), P("seq", "ch"), P("ch"), P(None, "ch"))
    return jax.shard_map(
        local_body, mesh=mesh, in_specs=placed, out_specs=P("seq", "ch"), check_vma=False
    )
```

```python
import functools
import math

import jax
import jax.numpy as jnp
from jax import lax
from jax.experimental import pallas as pl
from jax.experimental.pallas import tpu as pltpu
from jax.sharding import PartitionSpec as P

HIGHEST = lax.Precision.HIGHEST
MESH = pl.DeviceIdType.MESH
LANES = 128
TILE = 16
BUILD_UNROLL = 8
CONV_UNROLL = 16


def split_length(length):
    leading = 1
    for factor in range(1, math.isqrt(length) + 1):
        if length % factor == 0:
            leading = factor
    return (leading, length // leading)


def phase_table(count_rows, count_cols, modulus):
    row_ids = jnp.arange(count_rows, dtype=jnp.int32)
    col_ids = jnp.arange(count_cols, dtype=jnp.int32)
    wrapped = row_ids[:, None] * col_ids[None, :] % modulus
    phases = 2.0 * math.pi / modulus * wrapped.astype(jnp.float32)
    return (jnp.cos(phases), jnp.sin(phases))


def complex_form(cosine, sine):
    upper = jnp.stack([cosine, -sine], axis=1)
    lower = jnp.stack([sine, cosine], axis=1)
    return jnp.stack([upper, lower], axis=0)


def transform_tables(length):
    rows_lead, rows_tail = split_length(length)
    cos_lead, sin_lead = phase_table(rows_lead, rows_lead, rows_lead)
    cos_tail, sin_tail = phase_table(rows_tail, rows_tail, rows_tail)
    cos_twist, sin_twist = phase_table(rows_lead, rows_tail, length)
    lead_table = jnp.stack([cos_lead, -sin_lead])
    tail_forward = complex_form(cos_tail, -sin_tail)
    tail_inverse = complex_form(cos_tail, sin_tail)
    return (
        lead_table,
        tail_forward,
        tail_inverse,
        cos_twist,
        sin_twist,
        rows_lead,
        rows_tail,
        length,
    )


def twist_rows(section, cosine, sine):
    real_part = section[0] * cosine[None] - section[1] * sine[None]
    imag_part = section[0] * sine[None] + section[1] * cosine[None]
    return jnp.stack([real_part, imag_part])


def forward_rows(rows, tables):
    lead_table, tail_forward, tail_inverse, cos_twist, sin_twist, rows_lead, rows_tail, length = (
        tables
    )
    signal = jnp.concatenate([rows, jnp.zeros_like(rows)], axis=1).reshape(
        rows.shape[0], rows_lead, rows_tail
    )
    section = jnp.einsum("pft,cts->pcfs", lead_table, signal, precision=HIGHEST)
    twisted = twist_rows(section, cos_twist, -sin_twist)
    return jnp.einsum("pgrs,rcfs->pcfg", tail_forward, twisted, precision=HIGHEST)


def inverse_rows(spectrum, tables):
    lead_table, tail_forward, tail_inverse, cos_twist, sin_twist, rows_lead, rows_tail, length = (
        tables
    )
    section = jnp.einsum("pgrs,rcfs->pcfg", tail_inverse, spectrum, precision=HIGHEST)
    twisted = twist_rows(section, cos_twist, sin_twist)
    signal = jnp.einsum("rft,rcfs->cts", lead_table, twisted, precision=HIGHEST) / length
    return signal.reshape(signal.shape[0], length)


def product(left, right):
    real_part = left[0] * right[0] - left[1] * right[1]
    imag_part = left[0] * right[1] + left[1] * right[0]
    return jnp.stack([real_part, imag_part])


def body(values, gates, filter_taps, skip, out_weight):
    block_rows, width = values.shape
    whole_filter = lax.all_gather(filter_taps, "seq", axis=0, tiled=True)
    devices = lax.axis_size("seq")
    narrow = width // devices
    whole_rows = lax.all_to_all(values.T, "seq", split_axis=0, concat_axis=1, tiled=True)
    total_rows = whole_rows.shape[1]
    own_taps = lax.dynamic_slice_in_dim(whole_filter, lax.axis_index("seq") * narrow, narrow, 1).T
    used_taps = min(own_taps.shape[1], total_rows)
    own_taps = own_taps[:, :used_taps]
    taps_rows = jnp.concatenate(
        [own_taps, jnp.zeros((narrow, total_rows - used_taps), jnp.float32)], axis=1
    )
    row_tables = transform_tables(2 * total_rows)
    spectrum = product(forward_rows(whole_rows, row_tables), forward_rows(taps_rows, row_tables))
    convolved_rows = inverse_rows(spectrum, row_tables)[:, :total_rows]
    convolved = lax.all_to_all(convolved_rows, "seq", split_axis=1, concat_axis=0, tiled=True).T
    hidden = (gates * (convolved + skip[None, :] * values)).astype(jnp.bfloat16)
    return jnp.dot(
        lax.all_gather(hidden, "ch", axis=1, tiled=True),
        out_weight,
        preferred_element_type=jnp.float32,
    )


def toeplitz_kernel(
    tap_sources,
    values_hbm,
    gates_hbm,
    taps_hbm,
    skip_ref,
    weight_hbm,
    out_hbm,
    values_ref,
    gates_ref,
    taps_ref,
    out_ref,
    x_out,
    h_out,
    x_in,
    h_in,
    x_rows,
    toeplitz,
    h_blocks,
    y_blocks,
    y_out,
    y_in,
    hidden,
    weight,
    load_sem,
    out_sem,
    x_send,
    x_recv,
    h_send,
    h_recv,
    y_send,
    y_recv,
    g_send,
    g_recv,
):
    seq_size, narrow, block_rows = x_out.shape
    tap_rows = h_out.shape[2]
    ch_size, _, width = hidden.shape
    blocks = x_rows.shape[0] // narrow
    per = block_rows // LANES
    me, lane_group = lax.axis_index("seq"), lax.axis_index("ch")
    f32, bf16 = jnp.float32, jnp.bfloat16

    loads = [
        pltpu.make_async_copy(source, target, load_sem.at[place])
        for place, (source, target) in enumerate(
            (
                (values_hbm, values_ref),
                (taps_hbm, taps_ref),
                (gates_hbm, gates_ref),
                (weight_hbm, weight),
            )
        )
    ]
    for load in loads:
        load.start()

    barrier = pltpu.get_barrier_semaphore()
    for step in range(1, seq_size):
        pl.semaphore_signal(
            barrier, inc=1, device_id={"seq": lax.rem(me + step, seq_size)}, device_id_type=MESH
        )
    for step in range(1, ch_size):
        pl.semaphore_signal(
            barrier, inc=1, device_id={"ch": lax.rem(lane_group + step, ch_size)}, device_id_type=MESH
        )

    h_blocks[...] = jnp.zeros_like(h_blocks)
    loads[0].wait()
    x_out[...] = values_ref[...].T.astype(bf16).reshape(x_out.shape)
    pl.semaphore_wait(barrier, seq_size + ch_size - 2)

    groups = narrow // TILE
    x_copies = []
    for group in range(groups):
        part = pl.ds(group * TILE, TILE)
        for step in range(1, seq_size):
            to = lax.rem(me + step, seq_size)
            copy = pltpu.make_async_remote_copy(
                x_out.at[to, part], x_in.at[me, part],
                x_send.at[group, step], x_recv.at[group, step],
                device_id={"seq": to}, device_id_type=MESH,
            )
            copy.start()
            x_copies.append(copy)

    loads[1].wait()

    def tap_copy(group, step):
        to = lax.rem(me + step, seq_size)
        part = pl.ds(group * TILE, TILE)
        return pltpu.make_async_remote_copy(
            h_out.at[to, part], h_in.at[me, part], h_send.at[group, step], h_recv.at[group, me],
            device_id={"seq": to}, device_id_type=MESH,
        )

    @pl.when(me < tap_sources)
    def _():
        h_out[...] = taps_ref[...].T.astype(bf16).reshape(h_out.shape)
        for group in range(groups):
            for step in range(1, seq_size):
                tap_copy(group, step).start()
        h_in[me] = h_out[me]

    x_in[me] = x_out[me]
    row_ids = lax.broadcasted_iota(jnp.int32, (LANES, LANES), 0)
    col_ids = lax.broadcasted_iota(jnp.int32, (LANES, LANES), 1)

    def build_one(channel):
        before = jnp.zeros((LANES, LANES), f32)
        rows = x_rows[pl.ds(pl.multiple_of(channel * blocks, blocks), blocks), :]
        for block in range(blocks):
            row = rows[block : block + 1]
            turned = pltpu.roll(
                jnp.broadcast_to(row, (LANES, LANES)), 0, 1, stride=1, stride_axis=0
            )
            toeplitz[channel, block * LANES : (block + 1) * LANES, :] = jnp.where(
                col_ids >= row_ids, turned, before
            ).astype(bf16)
            before = turned

    def build(turn, carry):
        for part in range(BUILD_UNROLL):
            build_one(turn * BUILD_UNROLL + part)
        return carry

    turns = TILE // BUILD_UNROLL
    for group in range(groups):
        for copy in x_copies[group * (seq_size - 1) : (group + 1) * (seq_size - 1)]:
            copy.wait_recv()
        for source in range(seq_size):
            for piece in range(per):
                x_rows[pl.ds(group * TILE * blocks + source * per + piece, TILE, stride=blocks), :] = x_in[
                    source, group * TILE : (group + 1) * TILE, piece * LANES : (piece + 1) * LANES
                ].astype(f32)
        lax.fori_loop(group * turns, (group + 1) * turns, build, 0)

    pieces = tap_rows // LANES
    flat_blocks = h_blocks.reshape(narrow * 2 * blocks, LANES)

    def take_taps(group):
        part = slice(group * TILE, (group + 1) * TILE)
        for source in range(tap_sources):
            @pl.when(me != source)
            def _():
                pltpu.make_async_remote_copy(
                    h_out.at[0, part], h_in.at[source, part], h_send.at[group, 0],
                    h_recv.at[group, source], device_id={"seq": source}, device_id_type=MESH,
                ).wait_recv()
        for source in range(tap_sources):
            for piece in range(pieces):
                first = group * TILE * 2 * blocks + blocks + source * pieces + piece
                flat_blocks[pl.ds(first, TILE, stride=2 * blocks), :] = h_in[
                    source, part, piece * LANES : (piece + 1) * LANES
                ].astype(f32)

    def convolve_one(channel):
        left = jnp.concatenate(
            [h_blocks[channel, blocks - lag : 2 * blocks - lag, :] for lag in range(blocks)], axis=1
        ).astype(bf16)
        y_blocks[pl.ds(pl.multiple_of(channel * blocks, blocks), blocks), :] = jnp.dot(
            left, toeplitz[channel], preferred_element_type=f32
        )

    def convolve(turn, carry):
        for part in range(CONV_UNROLL):
            convolve_one(turn * CONV_UNROLL + part)
        return carry

    turns = TILE // CONV_UNROLL
    for group in range(groups):
        take_taps(group)
        lax.fori_loop(group * turns, (group + 1) * turns, convolve, 0)
    for block in range(blocks):
        y_out[block // per, :, (block % per) * LANES : (block % per + 1) * LANES] = y_blocks[
            pl.ds(block, narrow, stride=blocks), :
        ].astype(bf16)
    y_copies = {}
    for piece in range(per):
        span = pl.ds(piece * LANES, LANES)
        for step in range(1, seq_size):
            to = lax.rem(me + step, seq_size)
            y_copies[piece, step] = pltpu.make_async_remote_copy(
                y_out.at[to, :, span], y_in.at[me, :, span],
                y_send.at[piece, step], y_recv.at[piece, step],
                device_id={"seq": to}, device_id_type=MESH,
            )
            y_copies[piece, step].start()
    y_in[me] = y_out[me]

    partner = lane_group + 1 - 2 * lax.rem(lane_group, 2)
    pairs = ch_size // 2

    def spread(kind, piece, slot, to):
        block = hidden.at[slot, pl.ds(piece * LANES, LANES)]
        copy = pltpu.make_async_remote_copy(
            block, block, g_send.at[kind, piece], g_recv.at[kind, piece],
            device_id={"ch": to}, device_id_type=MESH,
        )
        copy.start()
        g_copies.append(copy)
        return copy

    def add_product(piece, slot, first=False):
        rows = slice(piece * LANES, (piece + 1) * LANES)
        term = jnp.dot(hidden[slot, rows], weight[slot], preferred_element_type=f32)
        out_ref[rows] = term if first else out_ref[rows] + term

    g_copies, direct, relayed = [], {}, {}
    loads[2].wait()
    for piece in range(per):
        rows = slice(piece * LANES, (piece + 1) * LANES)
        for step in range(1, seq_size):
            y_copies[piece, step].wait_recv()
        convolved = y_in[:, :, rows].astype(f32).reshape(width, LANES).T
        hidden[lane_group, rows] = (
            gates_ref[rows] * (convolved + skip_ref[...] * values_ref[rows])
        ).astype(bf16)
        for pair in range(1, pairs):
            direct[pair, piece] = spread(
                2 * pair - 1, piece, lane_group, lax.rem(lane_group + 2 * pair, ch_size)
            )
        direct[0, piece] = spread(0, piece, lane_group, partner)
    loads[3].wait()
    for piece in range(per):
        add_product(piece, lane_group, True)
    for piece in range(per):
        direct[0, piece].wait_recv()
        add_product(piece, partner)
    for piece in range(per):
        for pair in range(1, pairs):
            slot = lax.rem(lane_group + ch_size - 2 * pair, ch_size)
            direct[pair, piece].wait_recv()
            relayed[pair, piece] = spread(2 * pair, piece, slot, partner)
            add_product(piece, slot)
    stores = []
    for piece in range(per):
        rows = pl.ds(piece * LANES, LANES)
        for pair in range(1, pairs):
            slot = lax.rem(partner + ch_size - 2 * pair, ch_size)
            relayed[pair, piece].wait_recv()
            add_product(piece, slot)
        store = pltpu.make_async_copy(out_ref.at[rows], out_hbm.at[rows], out_sem.at[piece])
        store.start()
        stores.append(store)
    for store in stores:
        store.wait()

    for copy in x_copies + list(y_copies.values()) + g_copies:
        copy.wait_send()

    @pl.when(me < tap_sources)
    def _():
        for group in range(groups):
            for step in range(1, seq_size):
                tap_copy(group, step).wait_send()


def toeplitz_body(values, gates, filter_taps, skip, out_weight):
    seq_size, ch_size = lax.axis_size("seq"), lax.axis_size("ch")
    block_rows, width = values.shape
    tap_rows = filter_taps.shape[0]
    narrow = width // seq_size
    total = block_rows * seq_size
    sources = min(tap_rows * seq_size, total) // tap_rows
    columns = out_weight.shape[1]
    f32, bf16 = jnp.float32, jnp.bfloat16
    vmem = pl.BlockSpec(memory_space=pltpu.VMEM)
    hbm = pl.BlockSpec(memory_space=pl.ANY)
    per = block_rows // LANES
    dma = pltpu.SemaphoreType.DMA
    return pl.pallas_call(
        functools.partial(toeplitz_kernel, sources),
        out_shape=jax.ShapeDtypeStruct((block_rows, columns), f32),
        in_specs=[hbm] * 3 + [vmem, hbm],
        out_specs=hbm,
        scratch_shapes=[
            pltpu.VMEM((block_rows, width), f32),
            pltpu.VMEM((block_rows, width), f32),
            pltpu.VMEM((tap_rows, width), f32),
            pltpu.VMEM((block_rows, columns), f32),
            pltpu.VMEM((seq_size, narrow, block_rows), bf16),
            pltpu.VMEM((seq_size, narrow, tap_rows), bf16),
            pltpu.VMEM((seq_size, narrow, block_rows), bf16),
            pltpu.VMEM((sources, narrow, tap_rows), bf16),
            pltpu.VMEM((narrow * (total // LANES), LANES), f32),
            pltpu.VMEM((narrow, total, LANES), bf16),
            pltpu.VMEM((narrow, 2 * (total // LANES), LANES), f32),
            pltpu.VMEM((narrow * (total // LANES), LANES), f32),
            pltpu.VMEM((seq_size, narrow, block_rows), bf16),
            pltpu.VMEM((seq_size, narrow, block_rows), bf16),
            pltpu.VMEM((ch_size, block_rows, width), bf16),
            pltpu.VMEM((ch_size, width, columns), bf16),
            dma((4,)),
            dma((per,)),
            dma((narrow // TILE, seq_size)),
            dma((narrow // TILE, seq_size)),
            dma((narrow // TILE, seq_size)),
            dma((narrow // TILE, sources)),
            dma((per, seq_size)),
            dma((per, seq_size)),
            dma((ch_size, per)),
            dma((ch_size, per)),
        ],
        compiler_params=pltpu.CompilerParams(
            collective_id=0, has_side_effects=True, vmem_limit_bytes=63000 * 1024
        ),
    )(
        values,
        gates,
        filter_taps,
        skip.reshape(1, width),
        out_weight.reshape(ch_size, width, columns),
    )


def local_body(values, gates, filter_taps, skip, out_weight):
    seq_size = lax.axis_size("seq")
    block_rows, width = values.shape
    tap_rows = filter_taps.shape[0]
    narrow = width // seq_size
    total = block_rows * seq_size
    fits = (
        width % (seq_size * TILE) == 0
        and lax.axis_size("ch") % 2 == 0
        and width % LANES == 0
        and block_rows % LANES == 0
        and total // LANES % 8 == 0
        and tap_rows % LANES == 0
        and total % tap_rows == 0
        and narrow * total * LANES * 2 <= 32 * 1024 * 1024
    )
    chosen = toeplitz_body if fits else body
    return chosen(values, gates, filter_taps, skip, out_weight)


def solution(mesh):
    placed = (P("seq", "ch"), P("seq", "ch"), P("seq", "ch"), P("ch"), P(None, "ch"))
    return jax.shard_map(
        local_body, mesh=mesh, in_specs=placed, out_specs=P("seq", "ch"), check_vma=False
    )
```
